16 devices in a mesh: rep: 4 (over y, z, core), dp: 4 (over x).
Axes of the slice: x: 4, y: 2, z: 1, core: 2. Of those that a mesh axis runs over, the one named last changes fastest.
The devices are a block of a 4x4x8 slice.
Arguments:
- a: bfloat16 [16, 4, 4096, 896], P(('rep', 'dp')), parts along dimension 0
- g: bfloat16 [16, 4, 4096, 2560], P(('rep', 'dp')), parts along dimension 0
Outputs:
- output: bfloat16 [16, 896, 2560], P('rep'), parts along dimension 0
There are 4 independent parts. The reference program is written for one: setup_inputs(seed, part) draws one part's arguments, and reference() takes and returns one part's arrays. A program takes and returns all parts, laid end to end along the dimension named above; each array names one.
All inputs are finite; a program needn't handle non-finite values.
Results may differ from the reference program's by a relative error of at most 0.012.
Values are sent between devices in bfloat16 or wider.
A program may use at most 768 MiB of HBM per device.

```python
import jax
import jax.numpy as jnp
from jax import lax

DEVICES = 4
MATRICES = 4
TOKENS = 4096
D = 896
FF = 2560


def setup_inputs(seed: int = 0, part: int = 0) -> dict:
    ka, kg, ks = (jax.random.fold_in(k, part) for k in jax.random.split(jax.random.key(seed), 3))
    size = 2.0 ** jax.random.uniform(ks, (DEVICES, MATRICES, 1, 1), jnp.float32, -1.0, 1.0)
    a = jax.random.normal(ka, (DEVICES, MATRICES, TOKENS, D), jnp.float32)
    g = size * jax.random.normal(kg, (DEVICES, MATRICES, TOKENS, FF), jnp.float32) * (DEVICES * TOKENS) ** -0.5
    return {"a": a.astype(jnp.bfloat16), "g": g.astype(jnp.bfloat16)}


def reference(a, g):
    def take(so_far, one):
        return so_far + jnp.einsum("ntd,ntf->ndf", *one, preferred_element_type=jnp.float32), None

    return lax.scan(take, jnp.zeros((MATRICES, D, FF), jnp.float32), (a, g))[0].astype(jnp.bfloat16)
```

```python
import functools

import jax
import jax.numpy as jnp
from jax import lax
from jax.experimental import pallas as pl
from jax.experimental.pallas import tpu as pltpu
from jax.sharding import PartitionSpec as P

COLS = 256
HEAD = 128
ROWS = 448


def kernel(n, blocks, a_ref, g_ref, o_ref, at, gbuf, abuf, asem, gsem, ssem, rsem):
    mats, d, tokens = at.shape
    tiles = o_ref.shape[2] // COLS
    heads = d // HEAD
    slots = abuf.shape[0]
    me = lax.axis_index("dp")
    peers = (lax.rem(me + 1, n), lax.rem(me + n - 1, n))

    def unit(s, b, r):
        c = lax.rem(me + (2 * n - s if r == 0 else s), n)
        u = (b * 2 + r) * n + c
        j = lax.rem(u, tiles)
        return lax.div(u, tiles), pl.ds(pl.multiple_of(j * COLS, COLS), COLS)

    def send(s, b, r, rows=slice(None)):
        m, cols = unit(s, b, r)
        place = o_ref.at[m, rows, cols]
        return pltpu.make_async_remote_copy(
            src_ref=place,
            dst_ref=place,
            send_sem=ssem.at[s * blocks + b, r],
            recv_sem=rsem.at[s * blocks + b, r],
            device_id={"dp": peers[r]},
            device_id_type=pl.DeviceIdType.MESH,
        )

    def arrive(s, b, r):
        m, cols = unit(s + 1, b, r)
        place = o_ref.at[m, :, cols]
        pltpu.make_async_remote_copy(
            src_ref=place,
            dst_ref=place,
            send_sem=ssem.at[s * blocks + b, r],
            recv_sem=rsem.at[s * blocks + b, r],
            device_id={"dp": peers[r]},
            device_id_type=pl.DeviceIdType.MESH,
        ).wait_recv()

    def fetch_g(s, b, r, k):
        m, cols = unit(s, b, r)
        return pltpu.make_async_copy(g_ref.at[0, m, :, cols], gbuf.at[k], gsem.at[k])

    def fetch_a(q):
        m, i = lax.div(q, heads), lax.rem(q, heads)
        k = lax.rem(q, slots)
        rows = pl.ds(pl.multiple_of(i * HEAD, HEAD), HEAD)
        return pltpu.make_async_copy(a_ref.at[0, m, :, rows], abuf.at[k], asem.at[k])

    def piece(s, b, r, k, rows, add):
        m, cols = unit(s, b, r)
        total = jnp.dot(at[m, rows, :], gbuf[k], preferred_element_type=jnp.float32)
        if add:
            total += o_ref[m, rows, cols].astype(jnp.float32)
        o_ref[m, rows, cols] = total.astype(o_ref.dtype)

    barrier = pltpu.get_barrier_semaphore()
    for peer in peers:
        pl.semaphore_signal(
            barrier, inc=1, device_id={"dp": peer}, device_id_type=pl.DeviceIdType.MESH
        )
    fetch_a(0).start()
    for r in range(2):
        fetch_g(0, 0, r, r).start()
    for q in range(1, slots):
        fetch_a(q).start()
    pl.semaphore_wait(barrier, 2)

    last = mats * heads

    def first(b, _):
        k = lax.rem(b, 2) * 2
        for r in range(2):
            fetch_g(0, b + 1, r, 2 - k + r).start()
        for r in range(2):
            fetch_g(0, b, r, k + r).wait()

        def head(i, _):
            q = b * heads + i
            fetch_a(q).wait()
            rows = pl.ds(pl.multiple_of(i * HEAD, HEAD), HEAD)
            at[b, rows, :] = abuf[lax.rem(q, slots)].T

            @pl.when(q + slots < last)
            def _():
                fetch_a(q + slots).start()

            for r in range(2):
                piece(0, b, r, k + r, rows, False)
            for r in range(2):
                send(0, b, r, rows).start()
            return 0

        return lax.fori_loop(0, heads, head, 0)

    lax.fori_loop(0, mats, first, 0)

    def later(t, add, more):
        s, b = lax.div(t, blocks), lax.rem(t, blocks)
        k = lax.rem(t, 2) * 2

        def ahead():
            for r in range(2):
                s1, b1 = lax.div(t + 1, blocks), lax.rem(t + 1, blocks)
                fetch_g(s1, b1, r, 2 - k + r).start()

        if more is True:
            ahead()
        else:
            pl.when(more)(ahead)
        for r in range(2):
            fetch_g(s, b, r, k + r).wait()
            if add:
                arrive(s - 1, b, r)

            def part(i, _):
                piece(s, b, r, k + r, pl.ds(pl.multiple_of(i * ROWS, ROWS), ROWS), add)
                return 0

            lax.fori_loop(0, d // ROWS, part, 0)
            if add:
                send(s - 1, b, r).wait_send()
            send(s, b, r).start()

    for t in range(mats, blocks):
        later(jnp.int32(t), False, True)

    def reduce(t, _):
        later(t, True, t + 1 < n * blocks)
        return 0

    lax.fori_loop(blocks, n * blocks, reduce, 0)

    def gather(t, _):
        s, b = lax.div(t, blocks), lax.rem(t, blocks)
        for r in range(2):
            arrive(s - 1, b, r)
            send(s - 1, b, r).wait_send()
            send(s, b, r).start()
        return 0

    lax.fori_loop(n * blocks, (2 * n - 2) * blocks, gather, 0)

    def finish(b, _):
        for r in range(2):
            arrive(2 * n - 3, b, r)
            send(2 * n - 3, b, r).wait_send()
        return 0

    lax.fori_loop(0, blocks, finish, 0)


def solution(mesh):
    n = mesh.shape["dp"]

    def body(a, g):
        _, mats, tokens, d = a.shape
        ff = g.shape[3]
        blocks = mats * ff // COLS // (2 * n)
        return pl.pallas_call(
            functools.partial(kernel, n, blocks),
            out_shape=pltpu.VMEM((mats, d, ff), jnp.bfloat16),
            in_specs=[pl.BlockSpec(memory_space=pl.ANY)] * 2,
            out_specs=pl.BlockSpec(memory_space=pltpu.VMEM),
            scratch_shapes=[
                pltpu.VMEM((mats, d, tokens), jnp.bfloat16),
                pltpu.VMEM((4, tokens, COLS), jnp.bfloat16),
                pltpu.VMEM((3, tokens, HEAD), jnp.bfloat16),
                pltpu.SemaphoreType.DMA((3,)),
                pltpu.SemaphoreType.DMA((4,)),
                pltpu.SemaphoreType.DMA(((2 * n - 2) * blocks, 2)),
                pltpu.SemaphoreType.DMA(((2 * n - 2) * blocks, 2)),
            ],
            compiler_params=pltpu.CompilerParams(
                collective_id=0, has_side_effects=True, vmem_limit_bytes=44 * 2**20
            ),
        )(a, g)

    return jax.shard_map(
        body,
        mesh=mesh,
        in_specs=(P(("rep", "dp")), P(("rep", "dp"))),
        out_specs=P("rep"),
        check_vma=False,
    )
```

```python
import functools

import jax
import jax.numpy as jnp
from jax import lax
from jax.experimental import pallas as pl
from jax.experimental.pallas import tpu as pltpu
from jax.sharding import PartitionSpec as P

COLS = 256
HEAD = 128
ROWS = 448
SHARES = 4
LEFT = (4, 1)


def left_over():
    return LEFT[0] - (LEFT[0] - LEFT[1]) * lax.rem(lax.axis_index("rep"), 2)


def tile(n, tiles, me, s, b, r):
    c = lax.rem(me + 2 * n + (2 * r - 1) * s, n)
    u = (b * 2 + r) * n + c
    j = lax.rem(u, tiles)
    return lax.div(u, tiles), pl.ds(pl.multiple_of(j * COLS, COLS), COLS)


def reduce_and_gather(n, blocks, a_ref, g_ref, o_ref, at, gbuf, abuf, asem, gsem, fsem, ssem, rsem):
    mats, d, tokens = at.shape
    tiles = o_ref.shape[2] // COLS
    heads = d // HEAD
    slots = abuf.shape[0]
    me = lax.axis_index("dp")
    peers = [lax.rem(me + 1 + r * (n - 2), n) for r in range(2)]

    def unit(s, b, r):
        return tile(n, tiles, me, s, b, r)

    def send(s, b, r, rows=slice(None)):
        m, cols = unit(s, b, r)
        place = o_ref.at[m, rows, cols]
        return pltpu.make_async_remote_copy(
            src_ref=place,
            dst_ref=place,
            send_sem=ssem.at[s * blocks + b, r],
            recv_sem=rsem.at[s * blocks + b, r],
            device_id={"dp": lax.rem(me + 1 + r * (n - 2), n)},
            device_id_type=pl.DeviceIdType.MESH,
        )

    def arrive(s, b, r):
        m, cols = unit(s + 1, b, r)
        place = o_ref.at[m, :, cols]
        pltpu.make_async_remote_copy(
            src_ref=place,
            dst_ref=place,
            send_sem=ssem.at[s * blocks + b, r],
            recv_sem=rsem.at[s * blocks + b, r],
            device_id={"dp": peers[r]},
            device_id_type=pl.DeviceIdType.MESH,
        ).wait_recv()

    def fetch_g(s, b, r, k):
        m, cols = unit(s, b, r)
        return pltpu.make_async_copy(g_ref.at[0, m, :, cols], gbuf.at[k], gsem.at[k])

    def fetch_a(q):
        m, i = lax.div(q, heads), lax.rem(q, heads)
        k = lax.rem(q, slots)
        rows = pl.ds(pl.multiple_of(i * HEAD, HEAD), HEAD)
        return pltpu.make_async_copy(a_ref.at[0, m, :, rows], abuf.at[k], asem.at[k])

    def piece(s, b, r, k, rows, add):
        m, cols = unit(s, b, r)
        total = jnp.dot(at[m, rows, :], gbuf[k], preferred_element_type=jnp.float32)
        if add:
            total += o_ref[m, rows, cols].astype(jnp.float32)
        o_ref[m, rows, cols] = total.astype(o_ref.dtype)

    barrier = pltpu.get_barrier_semaphore()
    for peer in peers:
        pl.semaphore_signal(
            barrier, inc=1, device_id={"dp": peer}, device_id_type=pl.DeviceIdType.MESH
        )
    early = lax.rem(lax.axis_index("rep"), 2)
    m0, cols0 = unit(0, 0, early)
    shares = [pl.ds(i * (tokens // SHARES), tokens // SHARES) for i in range(SHARES)]
    first_a = [
        pltpu.make_async_copy(
            a_ref.at[0, 0, t, pl.ds(0, HEAD)], abuf.at[0, t], fsem.at[0, i]
        )
        for i, t in enumerate(shares)
    ]
    first_g = [
        pltpu.make_async_copy(g_ref.at[0, m0, t, cols0], gbuf.at[early, t], fsem.at[1, i])
        for i, t in enumerate(shares)
    ]
    for i in range(SHARES):
        first_a[i].start()
        first_g[i].start()

    last = mats * heads

    def turn(b, i):
        q = b * heads + i
        fetch_a(q).wait()
        rows = pl.ds(pl.multiple_of(i * HEAD, HEAD), HEAD)
        at[b, rows, :] = abuf[lax.rem(q, slots)].T

        @pl.when(q + slots < last)
        def _():
            fetch_a(q + slots).start()

        return rows

    def head(b, k, i):
        rows = turn(b, i)
        for r in range(2):
            piece(0, b, r, k + r, rows, False)
        for r in range(2):
            send(0, b, r, rows).start()
        return 0

    rows = pl.ds(0, HEAD)
    total = jnp.zeros((HEAD, COLS), jnp.float32)
    for i, t in enumerate(shares):
        first_a[i].wait()
        at[0, rows, t] = abuf[0, t].T
        first_g[i].wait()
        if i == 0:
            fetch_g(0, 0, 1 - early, 1 - early).start()
        if i == SHARES - 1:
            for q in range(1, slots):
                fetch_a(q).start()
        total += jnp.dot(at[0, rows, t], gbuf[early, t], preferred_element_type=jnp.float32)
    o_ref[m0, rows, cols0] = total.astype(o_ref.dtype)
    fetch_a(slots).start()
    pl.semaphore_wait(barrier, 2)
    send(0, 0, early, rows).start()
    fetch_g(0, 0, 1 - early, 1 - early).wait()
    piece(0, 0, 1 - early, 1 - early, rows, False)
    for r in range(2):
        fetch_g(0, 1, r, 2 + r).start()
    send(0, 0, 1 - early, rows).start()
    lax.fori_loop(1, heads, lambda i, _: head(jnp.int32(0), 0, i), 0)

    def first(b, _):
        k = lax.rem(b, 2) * 2
        for r in range(2):
            fetch_g(0, b + 1, r, 2 - k + r).start()
        for r in range(2):
            fetch_g(0, b, r, k + r).wait()
        return lax.fori_loop(0, heads, lambda i, _: head(b, k, i), 0)

    lax.fori_loop(1, mats, first, 0)

    def later(t, add, more):
        s, b = lax.div(t, blocks), lax.rem(t, blocks)
        k = lax.rem(t, 2) * 2

        def ahead():
            for r in range(2):
                s1, b1 = lax.div(t + 1, blocks), lax.rem(t + 1, blocks)
                fetch_g(s1, b1, r, 2 - k + r).start()

        if more is True:
            ahead()
        else:
            pl.when(more)(ahead)
        for r in range(2):
            fetch_g(s, b, r, k + r).wait()
            if add:
                arrive(s - 1, b, r)

            def part(i, _):
                piece(s, b, r, k + r, pl.ds(pl.multiple_of(i * ROWS, ROWS), ROWS), add)
                return 0

            lax.fori_loop(0, d // ROWS, part, 0)
            if add:
                send(s - 1, b, r).wait_send()
            send(s, b, r).start()

    for t in range(mats, blocks):
        later(jnp.int32(t), False, True)

    def reduce(t, _):
        later(t, True, t + 1 < n * blocks)
        return 0

    lax.fori_loop(blocks, n * blocks, reduce, 0)

    def gather(t, _):
        s, b = lax.div(t, blocks), lax.rem(t, blocks)
        for r in range(2):
            arrive(s - 1, b, r)
            send(s - 1, b, r).wait_send()
            send(s, b, r).start()
        return 0

    end = (2 * n - 2) * blocks - left_over()
    lax.fori_loop(n * blocks, end, gather, 0)

    def finish(t, _):
        s, b = lax.div(t, blocks), lax.rem(t, blocks)
        for r in range(2):
            arrive(s, b, r)
            send(s, b, r).wait_send()
        return 0

    lax.fori_loop(end - blocks, end, finish, 0)


def copy_out(o_ref, out_ref, sems):
    copies = [
        pltpu.make_async_copy(o_ref.at[m], out_ref.at[m], sems.at[m])
        for m in range(o_ref.shape[0])
    ]
    for copy in copies:
        copy.start()
    for copy in copies:
        copy.wait()


def last_hops(n, blocks, o_ref, _, p_ref, ssem, rsem):
    me = lax.axis_index("dp")
    peers = [lax.rem(me + 1 + r * (n - 2), n) for r in range(2)]
    barrier = pltpu.get_barrier_semaphore()
    for peer in peers:
        pl.semaphore_signal(
            barrier, inc=1, device_id={"dp": peer}, device_id_type=pl.DeviceIdType.MESH
        )
    pl.semaphore_wait(barrier, 2)

    def hop(b, r):
        m, cols = tile(n, o_ref.shape[2] // COLS, me, 2 * n - 3, b, r)
        return pltpu.make_async_remote_copy(
            src_ref=o_ref.at[m, :, cols],
            dst_ref=p_ref.at[b * 2 + r],
            send_sem=ssem.at[b, r],
            recv_sem=rsem.at[b, r],
            device_id={"dp": peers[r]},
            device_id_type=pl.DeviceIdType.MESH,
        )

    def start(b, _):
        for r in range(2):
            hop(b, r).start()
        return 0

    def wait(b, _):
        for r in range(2):
            hop(b, r).wait()
        return 0

    first = blocks - left_over()
    lax.fori_loop(first, blocks, start, 0)
    lax.fori_loop(first, blocks, wait, 0)


def copy_rest(n, blocks, p_ref, _, out_ref, sems):
    me = lax.axis_index("dp")

    def put(b, r):
        m, cols = tile(n, out_ref.shape[2] // COLS, me, 2 * n - 2, b, r)
        return pltpu.make_async_copy(
            p_ref.at[b * 2 + r], out_ref.at[m, :, cols], sems.at[b, r]
        )

    def start(b, _):
        for r in range(2):
            put(b, r).start()
        return 0

    def wait(b, _):
        for r in range(2):
            put(b, r).wait()
        return 0

    first = blocks - left_over()
    lax.fori_loop(first, blocks, start, 0)
    lax.fori_loop(first, blocks, wait, 0)


def solution(mesh):
    n = mesh.shape["dp"]

    def body(a, g):
        _, mats, tokens, d = a.shape
        ff = g.shape[3]
        blocks = mats * ff // COLS // (2 * n)
        hbm = pl.BlockSpec(memory_space=pltpu.HBM)
        vmem = pl.BlockSpec(memory_space=pltpu.VMEM)
        count = (2 * n - 2) * blocks
        sums = pl.pallas_call(
            functools.partial(reduce_and_gather, n, blocks),
            out_shape=pltpu.VMEM((mats, d, ff), jnp.bfloat16),
            in_specs=[hbm] * 2,
            out_specs=vmem,
            scratch_shapes=[
                pltpu.VMEM((mats, d, tokens), jnp.bfloat16),
                pltpu.VMEM((4, tokens, COLS), jnp.bfloat16),
                pltpu.VMEM((3, tokens, HEAD), jnp.bfloat16),
                pltpu.SemaphoreType.DMA((3,)),
                pltpu.SemaphoreType.DMA((4,)),
                pltpu.SemaphoreType.DMA((2, SHARES)),
                pltpu.SemaphoreType.DMA((count, 2)),
                pltpu.SemaphoreType.DMA((count, 2)),
            ],
            compiler_params=pltpu.CompilerParams(
                collective_id=0, has_side_effects=True, vmem_limit_bytes=44 * 2**20
            ),
        )(a, g)
        sums = pltpu.with_memory_space_constraint(sums, pltpu.VMEM)
        out = pl.pallas_call(
            copy_out,
            out_shape=jax.ShapeDtypeStruct((mats, d, ff), jnp.bfloat16),
            in_specs=[vmem],
            out_specs=hbm,
            scratch_shapes=[pltpu.SemaphoreType.DMA((mats,))],
            compiler_params=pltpu.CompilerParams(vmem_limit_bytes=2**20),
        )(sums)
        out = pltpu.with_memory_space_constraint(out, pltpu.HBM)
        rest = pl.pallas_call(
            functools.partial(last_hops, n, blocks),
            out_shape=pltpu.VMEM((blocks * 2, d, COLS), jnp.bfloat16),
            in_specs=[vmem, hbm],
            out_specs=vmem,
            scratch_shapes=[pltpu.SemaphoreType.DMA((blocks, 2))] * 2,
            compiler_params=pltpu.CompilerParams(
                collective_id=1, has_side_effects=True, vmem_limit_bytes=2**20
            ),
        )(sums, out)
        rest = pltpu.with_memory_space_constraint(rest, pltpu.VMEM)
        return pl.pallas_call(
            functools.partial(copy_rest, n, blocks),
            out_shape=jax.ShapeDtypeStruct((mats, d, ff), jnp.bfloat16),
            in_specs=[vmem, hbm],
            out_specs=hbm,
            input_output_aliases={1: 0},
            scratch_shapes=[pltpu.SemaphoreType.DMA((blocks, 2))],
            compiler_params=pltpu.CompilerParams(vmem_limit_bytes=2**20),
        )(rest, out)

    return jax.shard_map(
        body,
        mesh=mesh,
        in_specs=(P(("rep", "dp")), P(("rep", "dp"))),
        out_specs=P("rep"),
        check_vma=False,
    )
```

```python
import functools

import jax
import jax.numpy as jnp
from jax import lax
from jax.experimental import pallas as pl
from jax.experimental.pallas import tpu as pltpu
from jax.sharding import PartitionSpec as P

COLS = 256
HEAD = 128
ROWS = 448
SHARES = 4
LEFT = (1, 4)


def left_over():
    return LEFT[0] - (LEFT[0] - LEFT[1]) * lax.rem(lax.axis_index("rep"), 2)


def tile(n, tiles, me, s, b, r):
    c = lax.rem(me + 4 * n + (2 * r - 1) * s, n)
    u = (b * 2 + r) * n + c
    j = lax.rem(u, tiles)
    return lax.div(u, tiles), pl.ds(pl.multiple_of(j * COLS, COLS), COLS)


def reduce_and_gather(n, blocks, a_ref, g_ref, o_ref, at, gbuf, abuf, asem, gsem, fsem, ssem, rsem):
    mats, d, tokens = at.shape
    tiles = o_ref.shape[2] // COLS
    heads = d // HEAD
    slots = abuf.shape[0]
    me = lax.axis_index("dp")
    peers = [lax.rem(me + 1 + r * (n - 2), n) for r in range(2)]

    def unit(s, b, r):
        return tile(n, tiles, me, s, b, r)

    def send(s, b, r, rows=slice(None)):
        m, cols = unit(s, b, r)
        place = o_ref.at[m, rows, cols]
        return pltpu.make_async_remote_copy(
            src_ref=place,
            dst_ref=place,
            send_sem=ssem.at[s * blocks + b, r],
            recv_sem=rsem.at[s * blocks + b, r],
            device_id={"dp": lax.rem(me + 1 + r * (n - 2), n)},
            device_id_type=pl.DeviceIdType.MESH,
        )

    def arrive(s, b, r):
        m, cols = unit(s + 1, b, r)
        place = o_ref.at[m, :, cols]
        pltpu.make_async_remote_copy(
            src_ref=place,
            dst_ref=place,
            send_sem=ssem.at[s * blocks + b, r],
            recv_sem=rsem.at[s * blocks + b, r],
            device_id={"dp": peers[r]},
            device_id_type=pl.DeviceIdType.MESH,
        ).wait_recv()

    def fetch_g(s, b, r, k):
        m, cols = unit(s, b, r)
        return pltpu.make_async_copy(g_ref.at[0, m, :, cols], gbuf.at[k], gsem.at[k])

    def fetch_a(q):
        m, i = lax.div(q, heads), lax.rem(q, heads)
        k = lax.rem(q, slots)
        rows = pl.ds(pl.multiple_of(i * HEAD, HEAD), HEAD)
        return pltpu.make_async_copy(a_ref.at[0, m, :, rows], abuf.at[k], asem.at[k])

    def piece(s, b, r, k, rows, add):
        m, cols = unit(s, b, r)
        total = jnp.dot(at[m, rows, :], gbuf[k], preferred_element_type=jnp.float32)
        if add:
            total += o_ref[m, rows, cols].astype(jnp.float32)
        o_ref[m, rows, cols] = total.astype(o_ref.dtype)

    barrier = pltpu.get_barrier_semaphore()
    for peer in peers:
        pl.semaphore_signal(
            barrier, inc=1, device_id={"dp": peer}, device_id_type=pl.DeviceIdType.MESH
        )
    early = lax.rem(lax.axis_index("rep"), 2)
    m0, cols0 = unit(0, 0, early)
    shares = [pl.ds(i * (tokens // SHARES), tokens // SHARES) for i in range(SHARES)]
    first_a = [
        pltpu.make_async_copy(
            a_ref.at[0, 0, t, pl.ds(0, HEAD)], abuf.at[0, t], fsem.at[0, i]
        )
        for i, t in enumerate(shares)
    ]
    first_g = [
        pltpu.make_async_copy(g_ref.at[0, m0, t, cols0], gbuf.at[early, t], fsem.at[1, i])
        for i, t in enumerate(shares)
    ]
    for i in range(SHARES):
        first_a[i].start()
        first_g[i].start()

    last = mats * heads

    def turn(b, i):
        q = b * heads + i
        fetch_a(q).wait()
        rows = pl.ds(pl.multiple_of(i * HEAD, HEAD), HEAD)
        at[b, rows, :] = abuf[lax.rem(q, slots)].T

        @pl.when(q + slots < last)
        def _():
            fetch_a(q + slots).start()

        return rows

    def head(b, k, i):
        rows = turn(b, i)
        for r in range(2):
            piece(0, b, r, k + r, rows, False)
        for r in range(2):
            send(0, b, r, rows).start()
        return 0

    rows = pl.ds(0, HEAD)
    total = jnp.zeros((HEAD, COLS), jnp.float32)
    for i, t in enumerate(shares):
        first_a[i].wait()
        at[0, rows, t] = abuf[0, t].T
        first_g[i].wait()
        if i == 0:
            fetch_g(0, 0, 1 - early, 1 - early).start()
        if i == SHARES - 1:
            for q in range(1, slots):
                fetch_a(q).start()
        total += jnp.dot(at[0, rows, t], gbuf[early, t], preferred_element_type=jnp.float32)
    o_ref[m0, rows, cols0] = total.astype(o_ref.dtype)
    fetch_a(slots).start()
    pl.semaphore_wait(barrier, 2)
    send(0, 0, early, rows).start()
    fetch_g(0, 0, 1 - early, 1 - early).wait()
    piece(0, 0, 1 - early, 1 - early, rows, False)
    for r in range(2):
        fetch_g(0, 1, r, 2 + r).start()
    send(0, 0, 1 - early, rows).start()
    lax.fori_loop(1, heads, lambda i, _: head(jnp.int32(0), 0, i), 0)

    def first(b, _):
        k = lax.rem(b, 2) * 2
        for r in range(2):
            fetch_g(0, b + 1, r, 2 - k + r).start()
        for r in range(2):
            fetch_g(0, b, r, k + r).wait()
        return lax.fori_loop(0, heads, lambda i, _: head(b, k, i), 0)

    lax.fori_loop(1, mats, first, 0)

    def later(t, add, more):
        s, b = lax.div(t, blocks), lax.rem(t, blocks)
        k = lax.rem(t, 2) * 2

        def ahead():
            for r in range(2):
                s1, b1 = lax.div(t + 1, blocks), lax.rem(t + 1, blocks)
                fetch_g(s1, b1, r, 2 - k + r).start()

        if more is True:
            ahead()
        else:
            pl.when(more)(ahead)
        for r in range(2):
            fetch_g(s, b, r, k + r).wait()
            if add:
                arrive(s - 1, b, r)

            def part(i, _):
                piece(s, b, r, k + r, pl.ds(pl.multiple_of(i * ROWS, ROWS), ROWS), add)
                return 0

            lax.fori_loop(0, d // ROWS, part, 0)
            if add:
                send(s - 1, b, r).wait_send()
            send(s, b, r).start()

    for t in range(mats, blocks):
        later(jnp.int32(t), False, True)

    def reduce(t, _):
        later(t, True, t + 1 < n * blocks)
        return 0

    lax.fori_loop(blocks, n * blocks, reduce, 0)

    def gather(t, _):
        s, b = lax.div(t, blocks), lax.rem(t, blocks)
        for r in range(2):
            arrive(s - 1, b, r)
            send(s - 1, b, r).wait_send()
            send(s, b, r).start()
        return 0

    end = (2 * n - 2) * blocks - left_over()
    lax.fori_loop(n * blocks, end, gather, 0)

    def finish(t, _):
        s, b = lax.div(t, blocks), lax.rem(t, blocks)
        for r in range(2):
            arrive(s, b, r)
            send(s, b, r).wait_send()
        return 0

    lax.fori_loop(end - blocks, end, finish, 0)


def copy_out(n, blocks, o_ref, out_ref, sems):
    me = lax.axis_index("dp")
    first = blocks - left_over()

    def put(b, r, i):
        m, cols = tile(n, o_ref.shape[2] // COLS, me, 2 * n - 2 + i, b, r)
        return pltpu.make_async_copy(
            o_ref.at[m, :, cols], out_ref.at[m, :, cols], sems.at[b, r * n + i]
        )

    def each(which, act):
        def step(b, _):
            for r in range(2):
                for i in which:
                    act(put(b, r, i))
            return 0

        return step

    for act in (lambda copy: copy.start(), lambda copy: copy.wait()):
        lax.fori_loop(0, blocks, each(range(1, n), act), 0)
        lax.fori_loop(0, first, each(range(1), act), 0)


def last_hops(n, blocks, o_ref, _, p_ref, ssem, rsem):
    me = lax.axis_index("dp")
    peers = [lax.rem(me + 1 + r * (n - 2), n) for r in range(2)]
    barrier = pltpu.get_barrier_semaphore()
    for peer in peers:
        pl.semaphore_signal(
            barrier, inc=1, device_id={"dp": peer}, device_id_type=pl.DeviceIdType.MESH
        )
    pl.semaphore_wait(barrier, 2)

    def hop(b, r):
        m, cols = tile(n, o_ref.shape[2] // COLS, me, 2 * n - 3, b, r)
        return pltpu.make_async_remote_copy(
            src_ref=o_ref.at[m, :, cols],
            dst_ref=p_ref.at[b * 2 + r],
            send_sem=ssem.at[b, r],
            recv_sem=rsem.at[b, r],
            device_id={"dp": peers[r]},
            device_id_type=pl.DeviceIdType.MESH,
        )

    def start(b, _):
        for r in range(2):
            hop(b, r).start()
        return 0

    def wait(b, _):
        for r in range(2):
            hop(b, r).wait()
        return 0

    first = blocks - left_over()
    lax.fori_loop(first, blocks, start, 0)
    lax.fori_loop(first, blocks, wait, 0)


def copy_rest(n, blocks, p_ref, _, out_ref, sems):
    me = lax.axis_index("dp")

    def put(b, r):
        m, cols = tile(n, out_ref.shape[2] // COLS, me, 2 * n - 2, b, r)
        return pltpu.make_async_copy(
            p_ref.at[b * 2 + r], out_ref.at[m, :, cols], sems.at[b, r]
        )

    def start(b, _):
        for r in range(2):
            put(b, r).start()
        return 0

    def wait(b, _):
        for r in range(2):
            put(b, r).wait()
        return 0

    first = blocks - left_over()
    lax.fori_loop(first, blocks, start, 0)
    lax.fori_loop(first, blocks, wait, 0)


def solution(mesh):
    n = mesh.shape["dp"]

    def body(a, g):
        _, mats, tokens, d = a.shape
        ff = g.shape[3]
        blocks = mats * ff // COLS // (2 * n)
        hbm = pl.BlockSpec(memory_space=pltpu.HBM)
        vmem = pl.BlockSpec(memory_space=pltpu.VMEM)
        count = (2 * n - 2) * blocks
        sums = pl.pallas_call(
            functools.partial(reduce_and_gather, n, blocks),
            out_shape=pltpu.VMEM((mats, d, ff), jnp.bfloat16),
            in_specs=[hbm] * 2,
            out_specs=vmem,
            scratch_shapes=[
                pltpu.VMEM((mats, d, tokens), jnp.bfloat16),
                pltpu.VMEM((4, tokens, COLS), jnp.bfloat16),
                pltpu.VMEM((3, tokens, HEAD), jnp.bfloat16),
                pltpu.SemaphoreType.DMA((3,)),
                pltpu.SemaphoreType.DMA((4,)),
                pltpu.SemaphoreType.DMA((2, SHARES)),
                pltpu.SemaphoreType.DMA((count, 2)),
                pltpu.SemaphoreType.DMA((count, 2)),
            ],
            compiler_params=pltpu.CompilerParams(
                collective_id=0, has_side_effects=True, vmem_limit_bytes=44 * 2**20
            ),
        )(a, g)
        sums = pltpu.with_memory_space_constraint(sums, pltpu.VMEM)
        out = pl.pallas_call(
            functools.partial(copy_out, n, blocks),
            out_shape=jax.ShapeDtypeStruct((mats, d, ff), jnp.bfloat16),
            in_specs=[vmem],
            out_specs=hbm,
            scratch_shapes=[pltpu.SemaphoreType.DMA((blocks, 2 * n))],
            compiler_params=pltpu.CompilerParams(vmem_limit_bytes=2**20),
        )(sums)
        out = pltpu.with_memory_space_constraint(out, pltpu.HBM)
        rest = pl.pallas_call(
            functools.partial(last_hops, n, blocks),
            out_shape=pltpu.VMEM((blocks * 2, d, COLS), jnp.bfloat16),
            in_specs=[vmem, hbm],
            out_specs=vmem,
            scratch_shapes=[pltpu.SemaphoreType.DMA((blocks, 2))] * 2,
            compiler_params=pltpu.CompilerParams(
                collective_id=1, has_side_effects=True, vmem_limit_bytes=2**20
            ),
        )(sums, out)
        rest = pltpu.with_memory_space_constraint(rest, pltpu.VMEM)
        return pl.pallas_call(
            functools.partial(copy_rest, n, blocks),
            out_shape=jax.ShapeDtypeStruct((mats, d, ff), jnp.bfloat16),
            in_specs=[vmem, hbm],
            out_specs=hbm,
            input_output_aliases={1: 0},
            scratch_shapes=[pltpu.SemaphoreType.DMA((blocks, 2))],
            compiler_params=pltpu.CompilerParams(vmem_limit_bytes=2**20),
        )(rest, out)

    return jax.shard_map(
        body,
        mesh=mesh,
        in_specs=(P(("rep", "dp")), P(("rep", "dp"))),
        out_specs=P("rep"),
        check_vma=False,
    )
```

```python
import functools

import jax
import jax.numpy as jnp
from jax import lax
from jax.experimental import pallas as pl
from jax.experimental.pallas import tpu as pltpu
from jax.sharding import PartitionSpec as P

COLS = 256
HEAD = 128
ROWS = 448
SHARES = 4
LEFT = (1, 4)


def left_over():
    return LEFT[0] - (LEFT[0] - LEFT[1]) * lax.rem(lax.axis_index("rep"), 2)


def tile(n, tiles, me, s, b, r):
    c = lax.rem(me + 4 * n + (2 * r - 1) * s, n)
    u = (b * 2 + r) * n + c
    j = lax.rem(u, tiles)
    return lax.div(u, tiles), pl.ds(pl.multiple_of(j * COLS, COLS), COLS)


def reduce_and_gather(n, blocks, a_ref, g_ref, o_ref, at, gbuf, abuf, asem, gsem, fsem, ssem, rsem):
    mats, d, tokens = at.shape
    tiles = o_ref.shape[2] // COLS
    heads = d // HEAD
    slots = abuf.shape[0]
    me = lax.axis_index("dp")
    peers = [lax.rem(me + 1 + r * (n - 2), n) for r in range(2)]

    def unit(s, b, r):
        return tile(n, tiles, me, s, b, r)

    def send(s, b, r, rows=slice(None)):
        m, cols = unit(s, b, r)
        place = o_ref.at[m, rows, cols]
        return pltpu.make_async_remote_copy(
            src_ref=place,
            dst_ref=place,
            send_sem=ssem.at[s * blocks + b, r],
            recv_sem=rsem.at[s * blocks + b, r],
            device_id={"dp": lax.rem(me + 1 + r * (n - 2), n)},
            device_id_type=pl.DeviceIdType.MESH,
        )

    def arrive(s, b, r):
        m, cols = unit(s + 1, b, r)
        place = o_ref.at[m, :, cols]
        pltpu.make_async_remote_copy(
            src_ref=place,
            dst_ref=place,
            send_sem=ssem.at[s * blocks + b, r],
            recv_sem=rsem.at[s * blocks + b, r],
            device_id={"dp": peers[r]},
            device_id_type=pl.DeviceIdType.MESH,
        ).wait_recv()

    def fetch_g(s, b, r, k):
        m, cols = unit(s, b, r)
        return pltpu.make_async_copy(g_ref.at[0, m, :, cols], gbuf.at[k], gsem.at[k])

    def fetch_a(q):
        m, i = lax.div(q, heads), lax.rem(q, heads)
        k = lax.rem(q, slots)
        rows = pl.ds(pl.multiple_of(i * HEAD, HEAD), HEAD)
        return pltpu.make_async_copy(a_ref.at[0, m, :, rows], abuf.at[k], asem.at[k])

    def piece(s, b, r, k, rows, add):
        m, cols = unit(s, b, r)
        total = jnp.dot(at[m, rows, :], gbuf[k], preferred_element_type=jnp.float32)
        if add:
            total += o_ref[m, rows, cols].astype(jnp.float32)
        o_ref[m, rows, cols] = total.astype(o_ref.dtype)

    barrier = pltpu.get_barrier_semaphore()
    for peer in peers:
        pl.semaphore_signal(
            barrier, inc=1, device_id={"dp": peer}, device_id_type=pl.DeviceIdType.MESH
        )
    m0, cols0 = unit(0, 0, 0)
    shares = [pl.ds(i * (tokens // SHARES), tokens // SHARES) for i in range(SHARES)]
    first_a = [
        pltpu.make_async_copy(
            a_ref.at[0, 0, t, pl.ds(0, HEAD)], abuf.at[0, t], fsem.at[0, i]
        )
        for i, t in enumerate(shares)
    ]
    first_g = [
        pltpu.make_async_copy(g_ref.at[0, m0, t, cols0], gbuf.at[0, t], fsem.at[1, i])
        for i, t in enumerate(shares)
    ]
    for i in range(SHARES):
        first_a[i].start()
        first_g[i].start()
    fetch_g(0, 0, 1, 1).start()

    last = mats * heads

    def turn(b, i):
        q = b * heads + i
        fetch_a(q).wait()
        rows = pl.ds(pl.multiple_of(i * HEAD, HEAD), HEAD)
        at[b, rows, :] = abuf[lax.rem(q, slots)].T

        @pl.when(q + slots < last)
        def _():
            fetch_a(q + slots).start()

        return rows

    def head(b, k, i):
        rows = turn(b, i)
        for r in range(2):
            piece(0, b, r, k + r, rows, False)
        for r in range(2):
            send(0, b, r, rows).start()
        return 0

    rows = pl.ds(0, HEAD)
    total = jnp.zeros((HEAD, COLS), jnp.float32)
    for i, t in enumerate(shares):
        first_a[i].wait()
        at[0, rows, t] = abuf[0, t].T
        first_g[i].wait()
        if i == SHARES - 1:
            for q in range(1, slots):
                fetch_a(q).start()
        total += jnp.dot(at[0, rows, t], gbuf[0, t], preferred_element_type=jnp.float32)
    o_ref[m0, rows, cols0] = total.astype(o_ref.dtype)
    fetch_a(slots).start()
    pl.semaphore_wait(barrier, 2)
    send(0, 0, 0, rows).start()
    fetch_g(0, 0, 1, 1).wait()
    piece(0, 0, 1, 1, rows, False)
    for r in range(2):
        fetch_g(0, 1, r, 2 + r).start()
    send(0, 0, 1, rows).start()
    lax.fori_loop(1, heads, lambda i, _: head(jnp.int32(0), 0, i), 0)

    def first(b, _):
        k = lax.rem(b, 2) * 2
        for r in range(2):
            fetch_g(0, b + 1, r, 2 - k + r).start()
        for r in range(2):
            fetch_g(0, b, r, k + r).wait()
        return lax.fori_loop(0, heads, lambda i, _: head(b, k, i), 0)

    lax.fori_loop(1, mats, first, 0)

    def later(t, add, more):
        s, b = lax.div(t, blocks), lax.rem(t, blocks)
        k = lax.rem(t, 2) * 2

        def ahead():
            for r in range(2):
                s1, b1 = lax.div(t + 1, blocks), lax.rem(t + 1, blocks)
                fetch_g(s1, b1, r, 2 - k + r).start()

        if more is True:
            ahead()
        else:
            pl.when(more)(ahead)
        for r in range(2):
            fetch_g(s, b, r, k + r).wait()
            if add:
                arrive(s - 1, b, r)

            def part(i, _):
                piece(s, b, r, k + r, pl.ds(pl.multiple_of(i * ROWS, ROWS), ROWS), add)
                return 0

            lax.fori_loop(0, d // ROWS, part, 0)
            if add:
                send(s - 1, b, r).wait_send()
            send(s, b, r).start()

    for t in range(mats, blocks):
        later(jnp.int32(t), False, True)

    def reduce(t, _):
        later(t, True, t + 1 < n * blocks)
        return 0

    lax.fori_loop(blocks, n * blocks, reduce, 0)

    def gather(t, _):
        s, b = lax.div(t, blocks), lax.rem(t, blocks)
        for r in range(2):
            arrive(s - 1, b, r)
            send(s - 1, b, r).wait_send()
            send(s, b, r).start()
        return 0

    end = (2 * n - 2) * blocks - left_over()
    lax.fori_loop(n * blocks, end, gather, 0)

    def finish(t, _):
        s, b = lax.div(t, blocks), lax.rem(t, blocks)
        for r in range(2):
            arrive(s, b, r)
            send(s, b, r).wait_send()
        return 0

    lax.fori_loop(end - blocks, end, finish, 0)


def copy_out(n, blocks, o_ref, out_ref, sems):
    me = lax.axis_index("dp")
    first = blocks - left_over()

    def put(b, r, i):
        m, cols = tile(n, o_ref.shape[2] // COLS, me, 2 * n - 2 + i, b, r)
        return pltpu.make_async_copy(
            o_ref.at[m, :, cols], out_ref.at[m, :, cols], sems.at[b, r * n + i]
        )

    def each(which, act):
        def step(b, _):
            for r in range(2):
                for i in which:
                    act(put(b, r, i))
            return 0

        return step

    for act in (lambda copy: copy.start(), lambda copy: copy.wait()):
        lax.fori_loop(0, blocks, each(range(1, n), act), 0)
        lax.fori_loop(0, first, each(range(1), act), 0)


def last_hops(n, blocks, o_ref, _, p_ref, ssem, rsem):
    me = lax.axis_index("dp")
    peers = [lax.rem(me + 1 + r * (n - 2), n) for r in range(2)]
    barrier = pltpu.get_barrier_semaphore()
    for peer in peers:
        pl.semaphore_signal(
            barrier, inc=1, device_id={"dp": peer}, device_id_type=pl.DeviceIdType.MESH
        )
    pl.semaphore_wait(barrier, 2)

    def hop(b, r):
        m, cols = tile(n, o_ref.shape[2] // COLS, me, 2 * n - 3, b, r)
        return pltpu.make_async_remote_copy(
            src_ref=o_ref.at[m, :, cols],
            dst_ref=p_ref.at[b * 2 + r],
            send_sem=ssem.at[b, r],
            recv_sem=rsem.at[b, r],
            device_id={"dp": peers[r]},
            device_id_type=pl.DeviceIdType.MESH,
        )

    def start(b, _):
        for r in range(2):
            hop(b, r).start()
        return 0

    def wait(b, _):
        for r in range(2):
            hop(b, r).wait()
        return 0

    first = blocks - left_over()
    lax.fori_loop(first, blocks, start, 0)
    lax.fori_loop(first, blocks, wait, 0)


def copy_rest(n, blocks, p_ref, _, out_ref, sems):
    me = lax.axis_index("dp")

    def put(b, r):
        m, cols = tile(n, out_ref.shape[2] // COLS, me, 2 * n - 2, b, r)
        return pltpu.make_async_copy(
            p_ref.at[b * 2 + r], out_ref.at[m, :, cols], sems.at[b, r]
        )

    def start(b, _):
        for r in range(2):
            put(b, r).start()
        return 0

    def wait(b, _):
        for r in range(2):
            put(b, r).wait()
        return 0

    first = blocks - left_over()
    lax.fori_loop(first, blocks, start, 0)
    lax.fori_loop(first, blocks, wait, 0)


def solution(mesh):
    n = mesh.shape["dp"]

    def body(a, g):
        _, mats, tokens, d = a.shape
        ff = g.shape[3]
        blocks = mats * ff // COLS // (2 * n)
        hbm = pl.BlockSpec(memory_space=pltpu.HBM)
        vmem = pl.BlockSpec(memory_space=pltpu.VMEM)
        count = (2 * n - 2) * blocks
        sums = pl.pallas_call(
            functools.partial(reduce_and_gather, n, blocks),
            out_shape=pltpu.VMEM((mats, d, ff), jnp.bfloat16),
            in_specs=[hbm] * 2,
            out_specs=vmem,
            scratch_shapes=[
                pltpu.VMEM((mats, d, tokens), jnp.bfloat16),
                pltpu.VMEM((4, tokens, COLS), jnp.bfloat16),
                pltpu.VMEM((3, tokens, HEAD), jnp.bfloat16),
                pltpu.SemaphoreType.DMA((3,)),
                pltpu.SemaphoreType.DMA((4,)),
                pltpu.SemaphoreType.DMA((2, SHARES)),
                pltpu.SemaphoreType.DMA((count, 2)),
                pltpu.SemaphoreType.DMA((count, 2)),
            ],
            compiler_params=pltpu.CompilerParams(
                collective_id=0, has_side_effects=True, vmem_limit_bytes=44 * 2**20
            ),
        )(a, g)
        sums = pltpu.with_memory_space_constraint(sums, pltpu.VMEM)
        out = pl.pallas_call(
            functools.partial(copy_out, n, blocks),
            out_shape=jax.ShapeDtypeStruct((mats, d, ff), jnp.bfloat16),
            in_specs=[vmem],
            out_specs=hbm,
            scratch_shapes=[pltpu.SemaphoreType.DMA((blocks, 2 * n))],
            compiler_params=pltpu.CompilerParams(vmem_limit_bytes=2**20),
        )(sums)
        out = pltpu.with_memory_space_constraint(out, pltpu.HBM)
        rest = pl.pallas_call(
            functools.partial(last_hops, n, blocks),
            out_shape=pltpu.VMEM((blocks * 2, d, COLS), jnp.bfloat16),
            in_specs=[vmem, hbm],
            out_specs=vmem,
            scratch_shapes=[pltpu.SemaphoreType.DMA((blocks, 2))] * 2,
            compiler_params=pltpu.CompilerParams(
                collective_id=1, has_side_effects=True, vmem_limit_bytes=2**20
            ),
        )(sums, out)
        rest = pltpu.with_memory_space_constraint(rest, pltpu.VMEM)
        return pl.pallas_call(
            functools.partial(copy_rest, n, blocks),
            out_shape=jax.ShapeDtypeStruct((mats, d, ff), jnp.bfloat16),
            in_specs=[vmem, hbm],
            out_specs=hbm,
            input_output_aliases={1: 0},
            scratch_shapes=[pltpu.SemaphoreType.DMA((blocks, 2))],
            compiler_params=pltpu.CompilerParams(vmem_limit_bytes=2**20),
        )(rest, out)

    return jax.shard_map(
        body,
        mesh=mesh,
        in_specs=(P(("rep", "dp")), P(("rep", "dp"))),
        out_specs=P("rep"),
        check_vma=False,
    )
```
